64 devices in a mesh: dp: 4 (over x, y), ep: 16 (over z, core).
Axes of the slice: x: 2, y: 2, z: 8, core: 2. Of those that a mesh axis runs over, the one named last changes fastest.
The devices are a block of a 4x4x8 slice.
Arguments:
- x_tokens: bfloat16 [4096, 1536], P(('dp', 'ep')), parts along dimension 0
- slot_expert: int32 [320], replicated
- w1_slots: bfloat16 [320, 1536, 512], P('ep')
- w3_slots: bfloat16 [320, 1536, 512], P('ep')
- w2_slots: bfloat16 [320, 512, 1536], P('ep')
- assign: int32 [4096, 6], P(('dp', 'ep')), parts along dimension 0
- w_router: bfloat16 [1536, 64], replicated
- w1_shared: bfloat16 [1536, 1024], replicated
- w3_shared: bfloat16 [1536, 1024], replicated
- w2_shared: bfloat16 [1024, 1536], replicated
Outputs:
- output: bfloat16 [4096, 1536], P(('dp', 'ep')), parts along dimension 0
There are 4 independent parts. The reference program is written for one: setup_inputs(seed, part) draws one part's arguments, and reference() takes and returns one part's arrays. A program takes and returns all parts, laid end to end along the dimension named above; an argument that names none is the same for every part.
All inputs are finite; a program needn't handle non-finite values.
Results may differ from the reference program's by a relative error of at most 0.00102.
Values are sent between devices in bfloat16 or wider.
A program may use at most 768 MiB of HBM per device.

```python
import jax
import jax.numpy as jnp
from jax import lax

DIM_MODEL = 1536
FF_EXPERT = 512
FF_SHARED = 1024
NUM_EXPERTS = 64
TOP_K = 6
NUM_SLOTS = 320
GROUP_SIZE = 16
TOK_DEV = 64

TOKENS = TOK_DEV * GROUP_SIZE
CAP_ROWS = max(4, (3 * TOK_DEV * TOP_K) // NUM_SLOTS)
SEG_ROWS = min(TOKENS, GROUP_SIZE * CAP_ROWS)
ROUTE_SCALE = 2.5


def draw_routing(key_shared, key_part):
    key_rank, key_place = jax.random.split(key_shared, 2)
    rank_expert = jax.random.permutation(key_rank, NUM_EXPERTS).astype(jnp.int32)
    base_of_slot = jax.random.permutation(key_place, NUM_SLOTS).astype(jnp.int32)
    slot_expert = rank_expert[base_of_slot % NUM_EXPERTS]
    slot_of_base = jnp.argsort(base_of_slot).astype(jnp.int32)
    key_noise, key_coin, key_pick = jax.random.split(key_part, 3)
    rank_ids = jnp.arange(NUM_EXPERTS, dtype=jnp.int32)
    rank_bias = (2 * TOP_K * 4096) // (NUM_EXPERTS * (rank_ids + 1))
    noise_int = jax.random.randint(key_noise, (TOKENS, NUM_EXPERTS), 0, 4096, dtype=jnp.int32)
    token_ids = jnp.arange(TOKENS, dtype=jnp.int32)
    forced = token_ids < CAP_ROWS
    force_bonus = jnp.where(forced[:, None] & (rank_ids[None, :] == 0), 16384, 0)
    rank_score = (noise_int + rank_bias[None, :] + force_bonus) * NUM_EXPERTS + rank_ids[None, :]
    chosen_rank = lax.top_k(rank_score, TOP_K)[1].astype(jnp.int32)
    copies = (NUM_SLOTS - 1 - chosen_rank) // NUM_EXPERTS + 1
    coin_flip = jax.random.randint(key_coin, (TOKENS, TOP_K), 0, 2, dtype=jnp.int32)
    pick_copy = jax.random.randint(key_pick, (TOKENS, TOP_K), 0, 65536, dtype=jnp.int32) % copies
    keep_first = (coin_flip == 0) | (forced[:, None] & (chosen_rank == 0))
    copy_index = jnp.where(keep_first, 0, pick_copy)
    slot_pick = slot_of_base[chosen_rank + copy_index * NUM_EXPERTS]
    device_of = (token_ids // TOK_DEV)[:, None]
    group_key = (device_of * NUM_SLOTS + slot_pick).reshape(-1)
    sort_order = jnp.argsort(group_key, stable=True)
    sorted_key = group_key[sort_order]
    first_pos = jnp.searchsorted(sorted_key, sorted_key, side='left').astype(jnp.int32)
    rank_sorted = jnp.arange(TOKENS * TOP_K, dtype=jnp.int32) - first_pos
    rank_flat = jnp.zeros((TOKENS * TOP_K,), jnp.int32).at[sort_order].set(rank_sorted)
    assign = jnp.where(rank_flat < CAP_ROWS, slot_pick.reshape(-1), -1).reshape(TOKENS, TOP_K)
    return slot_expert, assign.astype(jnp.int32)


def setup_inputs(seed: int = 0, part: int = 0) -> dict:
    weight_keys = jax.random.split(jax.random.key(seed), 8)
    part_key = jax.random.fold_in(jax.random.key(seed + 1), part)
    key_tokens, key_route = jax.random.split(part_key, 2)
    slot_expert, assign = draw_routing(weight_keys[0], key_route)
    x_tokens = jax.random.normal(key_tokens, (TOKENS, DIM_MODEL), jnp.float32)
    w1_experts = jax.random.normal(weight_keys[1], (NUM_EXPERTS, DIM_MODEL, FF_EXPERT), jnp.float32) * DIM_MODEL ** -0.5
    w3_experts = jax.random.normal(weight_keys[2], (NUM_EXPERTS, DIM_MODEL, FF_EXPERT), jnp.float32) * DIM_MODEL ** -0.5
    w2_experts = jax.random.normal(weight_keys[3], (NUM_EXPERTS, FF_EXPERT, DIM_MODEL), jnp.float32) * FF_EXPERT ** -0.5
    w_router = jax.random.normal(weight_keys[4], (DIM_MODEL, NUM_EXPERTS), jnp.float32) * DIM_MODEL ** -0.5
    w1_shared = jax.random.normal(weight_keys[5], (DIM_MODEL, FF_SHARED), jnp.float32) * DIM_MODEL ** -0.5
    w3_shared = jax.random.normal(weight_keys[6], (DIM_MODEL, FF_SHARED), jnp.float32) * DIM_MODEL ** -0.5
    w2_shared = jax.random.normal(weight_keys[7], (FF_SHARED, DIM_MODEL), jnp.float32) * FF_SHARED ** -0.5
    return {
        'x_tokens': x_tokens.astype(jnp.bfloat16),
        'slot_expert': slot_expert,
        'w1_slots': w1_experts.astype(jnp.bfloat16)[slot_expert],
        'w3_slots': w3_experts.astype(jnp.bfloat16)[slot_expert],
        'w2_slots': w2_experts.astype(jnp.bfloat16)[slot_expert],
        'assign': assign,
        'w_router': w_router.astype(jnp.bfloat16),
        'w1_shared': w1_shared.astype(jnp.bfloat16),
        'w3_shared': w3_shared.astype(jnp.bfloat16),
        'w2_shared': w2_shared.astype(jnp.bfloat16),
    }


def gate_weights(x_tokens, assign, slot_expert, w_router):
    logits = jnp.dot(x_tokens, w_router, preferred_element_type=jnp.float32)
    gate_prob = jax.nn.sigmoid(logits)
    is_kept = assign >= 0
    chosen = slot_expert[jnp.maximum(assign, 0)]
    picked = jnp.where(is_kept, jnp.take_along_axis(gate_prob, chosen, axis=1), 0.0)
    gate_total = jnp.sum(picked, axis=1, keepdims=True)
    return ROUTE_SCALE * picked / jnp.maximum(gate_total, 1e-30), is_kept


def shared_expert(x_tokens, w1_shared, w3_shared, w2_shared):
    h_gate = jnp.dot(x_tokens, w1_shared, preferred_element_type=jnp.float32)
    h_up = jnp.dot(x_tokens, w3_shared, preferred_element_type=jnp.float32)
    mid_act = (jax.nn.silu(h_gate) * h_up).astype(jnp.bfloat16)
    return jnp.dot(mid_act, w2_shared, preferred_element_type=jnp.float32)


def reference(x_tokens, slot_expert, w1_slots, w3_slots, w2_slots, assign, w_router, w1_shared, w3_shared, w2_shared):
    route_weight, is_kept = gate_weights(x_tokens, assign, slot_expert, w_router)
    shared_out = shared_expert(x_tokens, w1_shared, w3_shared, w2_shared)
    flat_slot = jnp.where(is_kept, assign, NUM_SLOTS).reshape(-1)
    sort_order = jnp.argsort(flat_slot, stable=True)
    sorted_slot = flat_slot[sort_order]
    slot_ids = jnp.arange(NUM_SLOTS, dtype=jnp.int32)
    seg_start = jnp.searchsorted(sorted_slot, slot_ids, side='left').astype(jnp.int32)
    seg_end = jnp.searchsorted(sorted_slot, slot_ids, side='right').astype(jnp.int32)
    token_list = jnp.concatenate([(sort_order // TOP_K).astype(jnp.int32), jnp.zeros((SEG_ROWS,), jnp.int32)])
    weight_list = jnp.concatenate([route_weight.reshape(-1)[sort_order], jnp.zeros((SEG_ROWS,), route_weight.dtype)])
    row_offsets = jnp.arange(SEG_ROWS, dtype=jnp.int32)

    def slot_step(acc_rows, slot_id):
        seg_begin = seg_start[slot_id]
        row_ids = lax.dynamic_slice(token_list, (seg_begin,), (SEG_ROWS,))
        row_weight = lax.dynamic_slice(weight_list, (seg_begin,), (SEG_ROWS,))
        row_weight = jnp.where(row_offsets < seg_end[slot_id] - seg_begin, row_weight, 0.0)
        x_rows = x_tokens[row_ids]
        h_gate = jnp.dot(x_rows, w1_slots[slot_id], preferred_element_type=jnp.float32)
        h_up = jnp.dot(x_rows, w3_slots[slot_id], preferred_element_type=jnp.float32)
        mid_act = (jax.nn.silu(h_gate) * h_up).astype(jnp.bfloat16)
        out_rows = jnp.dot(mid_act, w2_slots[slot_id], preferred_element_type=jnp.float32).astype(jnp.bfloat16)
        acc_rows = acc_rows.at[row_ids].add(row_weight[:, None] * out_rows.astype(jnp.float32))
        return acc_rows, None

    routed = lax.scan(slot_step, jnp.zeros((TOKENS, DIM_MODEL), jnp.float32), slot_ids)[0]
    return (shared_out + routed).astype(jnp.bfloat16)
```

```python
import functools

import jax
import jax.numpy as jnp
from jax import lax
from jax.experimental import pallas as pl
from jax.experimental.pallas import tpu as pltpu
from jax.sharding import PartitionSpec as P

ROUTE_SCALE = 2.5
MESH = pl.DeviceIdType.MESH
F32 = jnp.float32
BF16 = jnp.bfloat16
RING = 9
QUOTA = {0: 12}
QUOTA_FAR = 4
CAPS = {0: 144, 1: 48, 2: 32, 3: 16, 4: 16}
FIT_STEPS = 8


def gate_weights(x_tokens, assign, slot_expert, w_router):
    logits = jnp.dot(x_tokens, w_router, preferred_element_type=jnp.float32)
    gate_prob = jax.nn.sigmoid(logits)
    is_kept = assign >= 0
    chosen = jnp.take(slot_expert, jnp.maximum(assign, 0))
    picked = jnp.where(is_kept, jnp.take_along_axis(gate_prob, chosen, axis=1), 0.0)
    gate_total = jnp.sum(picked, axis=1, keepdims=True)
    return ROUTE_SCALE * picked / jnp.maximum(gate_total, 1e-30), is_kept


def shared_expert(x_tokens, w1_shared, w3_shared, w2_shared):
    h_gate = jnp.dot(x_tokens, w1_shared, preferred_element_type=jnp.float32)
    h_up = jnp.dot(x_tokens, w3_shared, preferred_element_type=jnp.float32)
    mid_act = (jax.nn.silu(h_gate) * h_up).astype(jnp.bfloat16)
    return jnp.dot(mid_act, w2_shared, preferred_element_type=jnp.float32)


def plain_step(group_size, x_tokens, slot_expert, w1_slots, w3_slots, w2_slots, assign, w_router, w1_shared, w3_shared, w2_shared):
    tok_dev, dim_model = x_tokens.shape
    top_k = assign.shape[1]
    local_slots = w1_slots.shape[0]
    num_slots = local_slots * group_size
    cap_rows = max(4, (3 * tok_dev * top_k) // num_slots)
    route_weight, is_kept = gate_weights(x_tokens, assign, slot_expert, w_router)
    shared_out = shared_expert(x_tokens, w1_shared, w3_shared, w2_shared)
    flat_slot = jnp.where(is_kept, assign, num_slots).reshape(-1)
    onehot = (flat_slot[:, None] == jnp.arange(num_slots, dtype=jnp.int32)[None, :]).astype(jnp.int32)
    slot_rank = jnp.sum(jnp.cumsum(onehot, axis=0) * onehot, axis=1) - 1
    dummy_row = num_slots * cap_rows
    row_pos = jnp.where(flat_slot < num_slots, flat_slot * cap_rows + slot_rank, dummy_row)
    token_ids = jnp.arange(tok_dev * top_k, dtype=jnp.int32) // top_k
    row_token = jnp.full((dummy_row + 1,), tok_dev, jnp.int32).at[row_pos].set(token_ids)[:dummy_row]
    send_rows = jnp.take(x_tokens, row_token, axis=0, mode='fill', fill_value=0)
    recv_rows = lax.all_to_all(send_rows, 'ep', 0, 0, tiled=True)
    recv_rows = recv_rows.reshape(group_size, local_slots, cap_rows, dim_model)
    h_gate = jnp.einsum('jlcd,ldf->jlcf', recv_rows, w1_slots, preferred_element_type=jnp.float32)
    h_up = jnp.einsum('jlcd,ldf->jlcf', recv_rows, w3_slots, preferred_element_type=jnp.float32)
    mid_act = (jax.nn.silu(h_gate) * h_up).astype(jnp.bfloat16)
    expert_out = jnp.einsum('jlcf,lfd->jlcd', mid_act, w2_slots, preferred_element_type=jnp.float32).astype(jnp.bfloat16)
    back_rows = lax.all_to_all(expert_out.reshape(dummy_row, dim_model), 'ep', 0, 0, tiled=True)
    gathered = jnp.take(back_rows, jnp.minimum(row_pos, dummy_row - 1), axis=0).reshape(tok_dev, top_k, dim_model)
    routed = jnp.sum(route_weight[:, :, None] * gathered, axis=1)
    return (shared_out + routed).astype(jnp.bfloat16)


class Plan:
    def __init__(self, n, tok, top_k, slots):
        self.n, self.nz, self.tok, self.top_k, self.slots = n, n // 2, tok, top_k, slots
        nz = self.nz
        order = [0]
        for d in range(1, nz // 2):
            order += [d, nz - d]
        order.append(nz // 2)
        self.order = order
        self.blocks = [(d, f) for d in order for f in (0, 1)]
        self.pos = {b: i for i, b in enumerate(self.blocks)}
        self.ad = lambda d: min(d, nz - d)
        self.quota = [QUOTA.get(self.ad(d), QUOTA_FAR) for d, _ in self.blocks]
        self.cap = [CAPS[self.ad(d)] for d, _ in self.blocks]
        self.off = [sum(self.cap[:i]) for i in range(n)]
        self.rows = sum(self.cap)
        self.groups = n // 4
        self.grp_rows = [sum(self.quota[4 * g:4 * g + 4]) for g in range(self.groups)]
        self.grp_off = [sum(self.grp_rows[:g]) for g in range(self.groups)]
        self.m = sum(self.grp_rows)
        self.neg = [self.pos[((nz - d) % nz, f)] for d, f in self.blocks]


def iota(shape, dim):
    return lax.broadcasted_iota(jnp.int32, shape, dim)


def onehot(mask):
    return jnp.where(mask, 1.0, 0.0).astype(BF16)


def dot(a, b):
    return jnp.dot(a, b, preferred_element_type=F32)


def dot_nt(a, b):
    return lax.dot_general(a, b, (((1,), (1,)), ((), ())), preferred_element_type=F32)


def divmod_const(v, d):
    q = ((v.astype(F32) + 0.5) * (1.0 / d)).astype(jnp.int32)
    return q, v - q * d


def step_kernel(plan, n_dp, x_ref, assign_ref, se_row_ref, se_col_ref, wr_ref, w1_hbm, w3_hbm, w2_hbm, s1_hbm, s3_hbm, s2_hbm,
                y_ref, flag_ref, x_all, xo, ret, back, z_ref, meta, meta_all, flags, w1b, w3b, w2b,
                wsem, ring_s, ring_r, d2d_s, d2d_r, meta_s, meta_r, flag_s, flag_r, ret_s, ret_r):
    n, nz, tok, top_k, slots = plan.n, plan.nz, plan.tok, plan.top_k, plan.slots
    half = tok // 2
    dim = x_ref.shape[1]
    ff = w1b.shape[2]
    n_shared = s1_hbm.shape[1] // ff
    total = slots + n_shared
    me = lax.axis_index('ep')
    my_dp = lax.axis_index('dp')
    z, c = me // 2, lax.rem(me, 2)

    def dev_of(d, f):
        zz = lax.rem(z + d, nz)
        cc = c if f == 0 else 1 - c
        return zz * 2 + cc

    def peer(d, f):
        return {'dp': my_dp, 'ep': dev_of(d, f)}

    def weight_copies(v):
        b = v % RING
        if v < n_shared:
            cols = pl.ds(v * ff, ff)
            return [pltpu.make_async_copy(s1_hbm.at[:, cols], w1b.at[b], wsem.at[b, 0]),
                    pltpu.make_async_copy(s3_hbm.at[:, cols], w3b.at[b], wsem.at[b, 1]),
                    pltpu.make_async_copy(s2_hbm.at[cols, :], w2b.at[b], wsem.at[b, 2])]
        return slot_copies(v - n_shared, b)

    def slot_copies(s, b):
        return [pltpu.make_async_copy(w1_hbm.at[s], w1b.at[b], wsem.at[b, 0]),
                pltpu.make_async_copy(w3_hbm.at[s], w3b.at[b], wsem.at[b, 1]),
                pltpu.make_async_copy(w2_hbm.at[s], w2b.at[b], wsem.at[b, 2])]

    for v in range(RING):
        for cp in weight_copies(v):
            cp.start()

    barrier = pltpu.get_barrier_semaphore()
    for d, f in plan.blocks[1:]:
        pl.semaphore_signal(barrier, inc=1, device_id=peer(d, f), device_id_type=MESH)
    for g in range(1, n_dp):
        pl.semaphore_signal(barrier, inc=1, device_id={'dp': lax.rem(my_dp + g, n_dp), 'ep': me}, device_id_type=MESH)
    pl.semaphore_wait(barrier, n - 1 + n_dp - 1)

    def hcp(src, d, f, h, ss, rs, to):
        return pltpu.make_async_remote_copy(
            src_ref=src.at[pl.ds(h * half, half)], dst_ref=x_all.at[plan.pos[(d, f)], pl.ds(h * half, half)],
            send_sem=ss.at[d, h], recv_sem=rs.at[d, h], device_id=to, device_id_type=MESH)

    sib = peer(0, 1)
    right, left = peer(1, 0), peer(nz - 1, 0)
    mid = nz // 2
    sends = []

    def start(cp):
        cp.start()
        sends.append(cp)

    def from_left(hop):
        return nz - hop

    def ring_in(d):
        return x_all.at[plan.pos[(d, 0)]]

    def wait_in(d, f, h, ss, rs):
        hcp(x_ref, d, f, h, ss, rs, sib).wait_recv()

    for h in range(2):
        start(hcp(x_ref, from_left(1), 0, h, ring_s, ring_r, right))
        start(hcp(x_ref, 1, 0, h, ring_s, ring_r, left))
    for h in range(2):
        start(hcp(x_ref, 0, 1, h, d2d_s, d2d_r, sib))

    def ring_step(hop):
        for h in range(2):
            d = from_left(hop - 1)
            wait_in(d, 0, h, ring_s, ring_r)
            if hop < mid or h == 0:
                start(hcp(ring_in(d), from_left(hop), 0, h, ring_s, ring_r, right))
            start(hcp(ring_in(d), d, 1, h, d2d_s, d2d_r, sib))
            d = hop - 1
            wait_in(d, 0, h, ring_s, ring_r)
            if hop < mid or h == 1:
                start(hcp(ring_in(d), hop, 0, h, ring_s, ring_r, left))
            start(hcp(ring_in(d), d, 1, h, d2d_s, d2d_r, sib))

    nc = tok * top_k
    sp = se_row_ref.shape[1]
    x_own = x_ref[...]
    x_all[plan.pos[(0, 0)]] = x_own
    logits = dot(x_own, wr_ref[...])
    gate = jax.nn.sigmoid(logits)
    n_exp = gate.shape[1]
    assign = assign_ref[...]
    a_col = jnp.concatenate([assign[:, k:k + 1] for k in range(top_k)], axis=0)
    se_row = se_row_ref[...]
    se_col = se_col_ref[...]

    def slot_geometry(ids):
        dev, loc = divmod_const(ids, slots)
        dz = (dev >> 1) - z
        dz = jnp.where(dz < 0, dz + nz, dz)
        fl = (dev & 1) ^ c
        ad = jnp.minimum(dz, nz - dz)
        near = jnp.where(ad == 0, fl, ad + 1)
        key = (near * 512 + ((ids * 111 + me * 101) & 511)) * 512 + ids
        return dev, loc, dz, fl, ad, key

    id_row, id_col = iota((1, sp), 1), iota((sp, 1), 0)
    dev_r, loc_r, dz_r, fl_r, ad_r, key_r = slot_geometry(id_row)
    dev_c, _, _, _, _, key_c = slot_geometry(id_col)

    def by_ad(table, default):
        v = jnp.full((1, sp), default, F32)
        for a, t in table.items():
            v = jnp.where(ad_r == a, float(t), v)
        return v

    quota_r = by_ad(QUOTA, float(QUOTA_FAR))
    cap_r = by_ad(CAPS, 0.0)
    off_r = jnp.zeros((1, sp), F32)
    for i, (d, f) in enumerate(plan.blocks):
        off_r = jnp.where((dz_r == d) & (fl_r == f), float(plan.off[i] // 8), off_r)

    same = se_col == se_row
    same_m = onehot(same)
    near_m = onehot(same & (key_c < key_r))
    less_m = onehot((dev_c == dev_r) & (id_col < id_row))
    pick_s = onehot(a_col == id_row)
    rep = lambda v: jnp.broadcast_to(v, (8, sp))
    given = rep(jnp.sum(pick_s.astype(F32), axis=0, keepdims=True))
    n_r = dot(given.astype(BF16), same_m)
    e_c = dot_nt(pick_s, rep(se_row.astype(F32)).astype(BF16))[:, 0:1].astype(jnp.int32)
    kept_c = a_col >= 0
    e_c = jnp.where(kept_c, e_c, -1)
    hot_e = jnp.where(e_c == iota((nc, n_exp), 1), 1.0, 0.0)
    before = onehot(iota((nc, nc), 1) < iota((nc, nc), 0))
    r_c = jnp.sum(dot(before, hot_e.astype(BF16)) * hot_e, axis=1, keepdims=True)

    ring_step(2)

    lim = rep(quota_r)
    quota8, cap8 = lim, rep(cap_r)
    for _ in range(FIT_STEPS):
        cq = dot(lim.astype(BF16), near_m)
        cnt = jnp.clip(n_r - cq, 0.0, lim)
        base = dot(cnt.astype(BF16), less_m)
        lim = jnp.minimum(lim, jnp.maximum(cap8 - base, 0.0))
    cq = dot(lim.astype(BF16), near_m)
    cnt = jnp.clip(n_r - cq, 0.0, lim)
    base = dot(cnt.astype(BF16), less_m)
    over = jnp.max(jnp.where((cnt > 0.0) & (base + cnt > cap8), 1.0, 0.0))

    ring_step(3)

    cq1, lim1, base1 = cq[0:1], lim[0:1], base[0:1]
    sel = (e_c == se_row) & (r_c >= cq1) & (r_c < cq1 + lim1) & kept_c
    rows = [loc_r.astype(F32), dev_r.astype(F32), jnp.minimum(cq1, 128.0), jnp.minimum(base1, 256.0), off_r, jnp.ones((1, sp), F32)]
    row_i = iota((8, sp), 0)
    table = jnp.zeros((8, sp), F32)
    for i, r in enumerate(rows):
        table = jnp.where(row_i == i, r, table)
    val = dot_nt(onehot(sel), table.astype(BF16))
    loc_v, dev_v, cq_v, base_v, off_v, ok_v = [val[:, i:i + 1] for i in range(6)]
    placed = ok_v > 0.5
    r_in = r_c - cq_v
    code = jnp.where(placed, dev_v * 512.0 + loc_v * 16.0 + r_in, -1.0)
    q_c = jnp.where(placed, off_v * 8.0 + base_v + r_in, -1.0).astype(jnp.int32)
    lost = jnp.max(jnp.where(kept_c & jnp.logical_not(placed), 1.0, 0.0))
    my_flag = jnp.maximum(over, lost)

    lane = iota((tok, 128), 1)
    packed = jnp.full((tok, 128), -1.0, F32)
    for k in range(top_k):
        packed = jnp.where(lane == k, code[k * tok:(k + 1) * tok], packed)
    packed_t = jnp.transpose(packed)[0:8, :]
    meta[:, 0:tok] = jnp.where(iota((8, tok), 0) == 7, my_flag, packed_t)
    meta[:, tok:] = jnp.zeros((8, 128 - tok), F32)
    meta_all[0] = meta[...]

    picked = []
    for k in range(top_k):
        hot = hot_e[k * tok:(k + 1) * tok]
        picked.append(jnp.sum(hot * gate, axis=1, keepdims=True))
    gate_total = picked[0]
    for v in picked[1:]:
        gate_total = gate_total + v
    weight = [ROUTE_SCALE * v / jnp.maximum(gate_total, 1e-30) for v in picked]

    def meta_copy(i):
        d, f = plan.blocks[i]
        return pltpu.make_async_remote_copy(
            src_ref=meta, dst_ref=meta_all.at[plan.neg[i]], send_sem=meta_s.at[i], recv_sem=meta_r.at[plan.neg[i]],
            device_id=peer(d, f), device_id_type=MESH)

    for i in range(1, n):
        meta_copy(i).start()

    def wait_weights(b):
        for cp in slot_copies(0, b):
            cp.wait()

    def act(rows_, b):
        h1 = dot(rows_, w1b[b])
        h3 = dot(rows_, w3b[b])
        return (jax.nn.silu(h1) * h3).astype(BF16)

    for v in range(n_shared):
        for cp in weight_copies(v):
            cp.wait()
        part = dot(act(x_own, v), w2b[v])
        if v == 0:
            z_ref[...] = part
        else:
            z_ref[...] += part
        for cp in weight_copies(v + RING):
            cp.start()

    ring_step(4)
    for h in range(2):
        wait_in(mid, 0, h, ring_s, ring_r)
        start(hcp(ring_in(mid), mid, 1, h, d2d_s, d2d_r, sib))

    for i in range(1, n):
        meta_copy(plan.neg[i]).wait_recv()
    codes = [meta_all[i] for i in range(n)]
    grp_flag = codes[0]
    for i in range(1, n):
        grp_flag = jnp.maximum(grp_flag, codes[i])
    grp_flag = jnp.where(iota((8, 128), 0) == 7, grp_flag, 0.0)
    flags[0] = grp_flag

    def flag_copy(g):
        return pltpu.make_async_remote_copy(
            src_ref=flags.at[0], dst_ref=flags.at[g], send_sem=flag_s.at[g], recv_sem=flag_r.at[g],
            device_id={'dp': lax.rem(my_dp + g, n_dp), 'ep': me}, device_id_type=MESH)

    for d in plan.order:
        for h in range(2):
            wait_in(d, 1, h, d2d_s, d2d_r)

    sels = []
    for g in range(plan.groups):
        mg = plan.grp_rows[g]
        rr = iota((slots * mg, 1), 0)
        loc, w = divmod_const(rr, mg)
        parts = []
        lo = 0
        src_of = jnp.zeros((slots * mg, 1), jnp.int32)
        for i4 in range(4):
            i = 4 * g + i4
            inside = (w >= lo) & (w < lo + plan.quota[i])
            row_code = jnp.where(inside, loc * 16 + (w - lo), -7)
            src_of = jnp.where(inside, i4, src_of)
            cd = codes[i].astype(jnp.int32) - me * 512
            hit = jnp.zeros((slots * mg, tok), F32)
            for k in range(top_k):
                hit = jnp.where(row_code == cd[k:k + 1, 0:tok], 1.0, hit)
            parts.append(hit)
            lo += plan.quota[i]
        sel_g = jnp.concatenate(parts, axis=1).astype(BF16)
        xs = dot(sel_g, x_all[4 * g:4 * g + 4].reshape(4 * tok, dim))
        xo[:, plan.grp_off[g]:plan.grp_off[g] + mg, :] = xs.astype(BF16).reshape(slots, mg, dim)
        used = dot_nt(jnp.ones((8, 4 * tok), BF16), sel_g)
        sels.append(used)

    for g in range(1, n_dp):
        flag_copy(g).start()

    def slot_step(s, carry):
        v = s + n_shared
        b = lax.rem(v, RING)
        wait_weights(b)
        xo[s] = dot(act(xo[s], b), w2b[b]).astype(BF16)

        @pl.when(v + RING < total)
        def _():
            for cp in slot_copies(s + RING, b):
                cp.start()

        return carry

    lax.fori_loop(0, slots, slot_step, 0)

    def ret_copy(i):
        d, f = plan.blocks[i]
        j = plan.neg[i]
        return pltpu.make_async_remote_copy(
            src_ref=ret.at[pl.ds(plan.off[i], plan.cap[i])], dst_ref=back.at[pl.ds(plan.off[j], plan.cap[j])],
            send_sem=ret_s.at[i], recv_sem=ret_r.at[j], device_id=peer(d, f), device_id_type=MESH)

    for g in range(plan.groups - 1, -1, -1):
        mg = plan.grp_rows[g]
        rows_g = slots * mg
        lo = [sum(plan.quota[4 * g:4 * g + i4]) for i4 in range(5)]

        def source(v):
            _, w = divmod_const(v, mg)
            src = jnp.zeros(v.shape, jnp.int32)
            for i4 in range(1, 4):
                src = jnp.where(w >= lo[i4], i4, src)
            return src

        r_row, r_col = iota((1, rows_g), 1), iota((rows_g, 1), 0)
        s_row, s_col = source(r_row), source(r_col)
        prefix = onehot((s_col == s_row) & (r_col < r_row))
        used = sels[g]
        p_row = dot(used.astype(BF16), prefix)[0:1]
        used_row = used[0:1]
        c0 = plan.off[4 * g]
        cg = sum(plan.cap[4 * g:4 * g + 4])
        q_col = iota((cg, 1), 0)
        src_q = jnp.zeros((cg, 1), jnp.int32)
        base_q = jnp.zeros((cg, 1), jnp.int32)
        for i4 in range(1, 4):
            o = plan.off[4 * g + i4] - c0
            src_q = jnp.where(q_col >= o, i4, src_q)
            base_q = jnp.where(q_col >= o, o, base_q)
        pick = onehot((p_row.astype(jnp.int32) == q_col - base_q) & (src_q == s_row) & (used_row > 0.5))
        o_g = xo[:, plan.grp_off[g]:plan.grp_off[g] + mg, :].reshape(rows_g, dim)
        out = dot(pick, o_g).astype(BF16)
        ret[c0:c0 + cg, :] = out
        if g == 0:
            back[0:plan.cap[0], :] = out[0:plan.cap[0]]
        for i in range(4 * g, 4 * g + 4):
            if i > 0:
                ret_copy(i).start()

    q_iota = iota((1, plan.rows), 1)
    take = onehot(q_c == q_iota)

    for cp in sends:
        cp.wait_send()
    for i in range(1, n):
        meta_copy(i).wait_send()
    for g in range(1, n_dp):
        flag_copy(g).wait()
    flag = flags[0]
    for g in range(1, n_dp):
        flag = jnp.maximum(flag, flags[g])
    flag_ref[...] = flag

    for i in range(1, n):
        ret_copy(plan.neg[i]).wait_recv()
    step = 256
    for j in range(0, dim, step):
        got = dot(take, back[:, j:j + step])
        acc = z_ref[:, j:j + step]
        tot = weight[0] * got[0:tok]
        for k in range(1, top_k):
            tot = tot + weight[k] * got[k * tok:(k + 1) * tok]
        y_ref[:, j:j + step] = (acc + tot).astype(BF16)
    for i in range(1, n):
        ret_copy(i).wait_send()


def fast_step(n, n_dp, x, slot_expert, w1, w3, w2, assign, w_router, s1, s3, s2):
    tok, dim = x.shape
    slots, _, ff = w1.shape
    plan = Plan(n, tok, assign.shape[1], slots)
    num = slots * n
    sp = -(-num // 128) * 128
    se = jnp.pad(slot_expert, (0, sp - num), constant_values=-2)
    vmem = pl.BlockSpec(memory_space=pltpu.VMEM)
    anym = pl.BlockSpec(memory_space=pl.ANY)
    dma, sh = pltpu.SemaphoreType.DMA, (plan.nz, 2)
    return pl.pallas_call(
        functools.partial(step_kernel, plan, n_dp),
        out_shape=(jax.ShapeDtypeStruct((tok, dim), BF16), jax.ShapeDtypeStruct((8, 128), F32)),
        in_specs=[vmem] * 5 + [anym] * 6,
        out_specs=(vmem, vmem),
        scratch_shapes=[
            pltpu.VMEM((n, tok, dim), BF16),
            pltpu.VMEM((slots, plan.m, dim), BF16),
            pltpu.VMEM((plan.rows, dim), BF16),
            pltpu.VMEM((plan.rows, dim), BF16),
            pltpu.VMEM((tok, dim), F32),
            pltpu.VMEM((8, 128), F32),
            pltpu.VMEM((n, 8, 128), F32),
            pltpu.VMEM((n_dp, 8, 128), F32),
            pltpu.VMEM((RING, dim, ff), BF16),
            pltpu.VMEM((RING, dim, ff), BF16),
            pltpu.VMEM((RING, ff, dim), BF16),
            dma((RING, 3)), dma(sh), dma(sh), dma(sh), dma(sh), dma((n,)), dma((n,)), dma((n_dp,)), dma((n_dp,)), dma((n,)), dma((n,)),
        ],
        compiler_params=pltpu.CompilerParams(collective_id=0, has_side_effects=True, vmem_limit_bytes=64 * 1024 * 1024 - 65536),
    )(x, assign, se.reshape(1, sp), se.reshape(sp, 1), w_router, w1, w3, w2, s1, s3, s2)


def solution(mesh):
    n, n_dp = mesh.shape['ep'], mesh.shape['dp']

    def device_step(*args):
        y, flag = fast_step(n, n_dp, *args)
        return lax.cond(jnp.max(flag) > 0.5, lambda: plain_step(n, *args), lambda: y)

    token_spec = P(('dp', 'ep'), None)
    slot_spec = P('ep', None, None)
    return jax.shard_map(device_step, mesh=mesh, in_specs=(token_spec, P(), slot_spec, slot_spec, slot_spec, token_spec, P(), P(), P(), P()), out_specs=token_spec, check_vma=False)
```
